32 devices in a mesh: group: 8 (over z, x), shard: 4 (over y, core).
Axes of the slice: x: 2, y: 2, z: 4, core: 2. Of those that a mesh axis runs over, the one named last changes fastest.
Arguments:
- tokens: bfloat16 [4096, 4096], P(('group', 'shard')), may hold values from -12 to 12
- out_grad: bfloat16 [4096, 4096], P(('group', 'shard')), may hold values from -12 to 12
- expert_ids: int32 [4096, 2], P(('group', 'shard')), may hold values from 0 to 7, as said below
- route_weights: bfloat16 [4096, 2], P(('group', 'shard')), may hold values from 0.099609375 to 1
- w_gate: bfloat16 [4096, 7168], P(None, 'shard'), may hold values from -0.09375 to 0.09375
- w_up: bfloat16 [4096, 7168], P(None, 'shard'), may hold values from -0.09375 to 0.09375
- w_down: bfloat16 [7168, 4096], P('shard'), may hold values from -0.0625 to 0.0625
Outputs:
- token_grad: bfloat16 [4096, 4096], P(('group', 'shard'))
- route_grad: float32 [4096, 2], P(('group', 'shard'))
- grad_gate: bfloat16 [4096, 7168], P('group', 'shard')
- grad_up: bfloat16 [4096, 7168], P('group', 'shard')
- grad_down: bfloat16 [7168, 4096], P('shard', 'group')
- grad_rms: float32 [], replicated
The draws below stay inside these ranges and needn't reach their ends.
Inputs may be any that keep to these rules, and one draw needn't show every extreme that they name: `expert_ids`: each row names two different experts. Of the 128 rows of one device, at least 12 and at most 48 name expert 0; in every draw all devices of one index of group have exactly 48 such rows.
All inputs are finite; a program needn't handle non-finite values.
Results may differ from the reference program's by a relative error of at most 0.017.
Values may be sent and summed in bfloat16 or wider, within the bound.
A program may use at most 192 MiB of HBM per device.

```python
import math
import jax
import jax.numpy as jnp
from jax import lax

D = 4096
FF = 7168
EXPERTS = 8
TOK_DEV = 128
CAP = 48
TOKENS = 4096
N_GROUP = 8
N_SHARD = 4


def column_field(key, row_total, column_total):
    key_jitter, key_base = jax.random.split(key, 2)
    column_ramp = 3.0 ** (jnp.arange(column_total, dtype=jnp.float32) / column_total)
    jitter = jnp.exp(jax.random.uniform(key_jitter, (column_total,), jnp.float32, 0.0, 1.2))
    values = jax.random.normal(key_base, (row_total, column_total), jnp.float32)
    values = jnp.clip(values, -6.0, 6.0)
    return jnp.clip(0.5 * values * column_ramp * jitter, -12.0, 12.0)


def draw_tokens(key, part):
    return column_field(jax.random.fold_in(key, 11), TOKENS, D).astype(jnp.bfloat16)


def draw_out_grad(key, part):
    return column_field(jax.random.fold_in(key, 17), TOKENS, D).astype(jnp.bfloat16)


def block_ranks(block_key):
    return jax.random.permutation(block_key, TOK_DEV)


def draw_expert_ids(key, part):
    blocks = TOKENS // TOK_DEV
    key_counts, key_full, key_ranks, key_first, key_offset, key_flip = jax.random.split(jax.random.fold_in(key, 23), 6)
    counts = jax.random.randint(key_counts, (blocks,), max(CAP // 4, 1), CAP + 1)
    full_group = jax.random.randint(key_full, (), 0, blocks // N_SHARD)
    counts = jnp.where(jnp.arange(blocks) // N_SHARD == full_group, CAP, counts)
    row_ranks = jax.vmap(block_ranks)(jax.random.split(key_ranks, blocks))
    routed = (row_ranks < counts[:, None]).reshape(TOKENS)
    first_pick = jax.random.randint(key_first, (TOKENS,), 1, EXPERTS)
    offset_pick = jax.random.randint(key_offset, (TOKENS,), 1, EXPERTS - 1)
    second = 1 + (first_pick - 1 + offset_pick) % (EXPERTS - 1)
    lead_pick = jnp.where(routed, 0, second)
    flipped = jax.random.randint(key_flip, (TOKENS,), 0, 2) == 1
    left_pick = jnp.where(flipped, first_pick, lead_pick)
    right_pick = jnp.where(flipped, lead_pick, first_pick)
    return jnp.stack([left_pick, right_pick], axis=1).astype(jnp.int32)


def level_of(key, dims, cuts, least, largest):
    level, own = 1.0, jax.random.fold_in(key, 6)
    for axis_at, blocks in cuts:
        steps = jnp.exp(jax.random.uniform(jax.random.fold_in(own, axis_at), (blocks,), jnp.float32, least / len(cuts), largest / len(cuts)))
        level = level * jnp.repeat(steps, dims[axis_at] // blocks).reshape([-1 if axis == axis_at else 1 for axis in range(len(dims))])
    return level


def gaussian(key, extent, spread, bound, shards=(), kind=jnp.bfloat16):
    level = level_of(key, extent, shards, -0.22, 0.18) if shards else 1.0
    entries = jax.random.normal(key, extent, jnp.float32) * spread * level
    return jnp.minimum(jnp.maximum(entries, -bound), bound).astype(kind)


def setup_inputs(seed: int = 0) -> dict:
    splits = jax.random.split(jax.random.key(seed), 8)
    tokens = draw_tokens(jax.random.fold_in(splits[7], 71), 0)
    out_grad = draw_out_grad(jax.random.fold_in(splits[7], 71), 0)
    expert_ids = draw_expert_ids(jax.random.fold_in(splits[7], 71), 0)
    route_weights = jnp.clip(jnp.exp(math.log(1.0) - 2.306499 * jax.random.uniform(splits[3], (TOKENS, 2), jnp.float32) ** level_of(splits[3], (TOKENS, 2), ((0, 32),), -0.2, 0.2)), 0.099609375, 1.0).astype(jnp.bfloat16)
    w_gate = gaussian(splits[4], (D, FF), D ** -0.5, 0.09375, ((1, 4),))
    w_up = gaussian(splits[5], (D, FF), D ** -0.5, 0.09375, ((1, 4),))
    w_down = gaussian(splits[6], (FF, D), FF ** -0.5, 0.0625, ((0, 4),))
    return dict(tokens=tokens, out_grad=out_grad, expert_ids=expert_ids, route_weights=route_weights, w_gate=w_gate, w_up=w_up, w_down=w_down)


def pack_block(ids_block, weights_block):
    expert_hits = ids_block == 0
    routed = jnp.any(expert_hits, axis=1)
    weight = lax.optimization_barrier(jnp.sum(jnp.where(expert_hits, weights_block.astype(jnp.float32), jnp.float32(0.0)), axis=1))
    slot_order = jnp.cumsum(routed.astype(jnp.int32)) - 1
    slot_index = lax.broadcasted_iota(jnp.int32, (CAP, ids_block.shape[0]), 0)
    placing = jnp.logical_and(slot_order[None, :] == slot_index, routed[None, :]).astype(jnp.float32)
    return (expert_hits, placing, weight)

def rounded(value):
    return lax.optimization_barrier(value.astype(jnp.bfloat16)).astype(jnp.float32)

def reference(tokens, out_grad, expert_ids, route_weights, w_gate, w_up, w_down):
    row_total = N_SHARD * CAP
    tokens_grouped = tokens.reshape(N_GROUP, N_SHARD, TOK_DEV, D)
    grads_grouped = out_grad.reshape(N_GROUP, N_SHARD, TOK_DEV, D)
    ids_grouped = expert_ids.reshape(N_GROUP, N_SHARD, TOK_DEV, 2)
    weights_grouped = route_weights.reshape(N_GROUP, N_SHARD, TOK_DEV, 2)

    def one_group(totals, group_data):
        group_x, group_dy, group_ids, group_weights = group_data
        expert_hits, placing, weight = jax.vmap(pack_block)(group_ids, group_weights)
        rows_x = jnp.einsum('sct,std->scd', placing, group_x.astype(jnp.float32)).astype(jnp.bfloat16).reshape(row_total, D)
        rows_dy = jnp.einsum('sct,std->scd', placing, group_dy.astype(jnp.float32)).astype(jnp.bfloat16).reshape(row_total, D)
        rows_route = lax.optimization_barrier(jnp.sum(placing * weight[:, None, :], axis=2)).reshape(row_total, 1)
        gate_pre = jnp.dot(rows_x, w_gate, preferred_element_type=jnp.float32)
        up_pre = jnp.dot(rows_x, w_up, preferred_element_type=jnp.float32)
        hidden_grad = jnp.dot(rows_dy, w_down.T, preferred_element_type=jnp.float32)
        sigmoid_gate = jax.nn.sigmoid(gate_pre)
        activated = gate_pre * sigmoid_gate
        hidden = activated * up_pre
        route_part = lax.optimization_barrier(jnp.sum(hidden * hidden_grad, axis=1))
        weighted_hidden = (rows_route * hidden).astype(jnp.bfloat16)
        gate_grad = (rows_route * hidden_grad * up_pre * sigmoid_gate * (1.0 + gate_pre * (1.0 - sigmoid_gate))).astype(jnp.bfloat16)
        up_grad = (rows_route * hidden_grad * activated).astype(jnp.bfloat16)
        row_grads = (jnp.dot(gate_grad, w_gate.T, preferred_element_type=jnp.float32) + jnp.dot(up_grad, w_up.T, preferred_element_type=jnp.float32)).astype(jnp.bfloat16)
        token_block = jnp.einsum('sct,scd->std', placing, row_grads.reshape(N_SHARD, CAP, D).astype(jnp.float32)).astype(jnp.bfloat16)
        route_tok = jnp.einsum('sct,sc->st', placing, route_part.reshape(N_SHARD, CAP))
        route_block = jnp.where(expert_hits, route_tok[:, :, None], jnp.float32(0.0))
        part_gate = rounded(jnp.dot(rows_x.T, gate_grad, preferred_element_type=jnp.float32))
        part_up = rounded(jnp.dot(rows_x.T, up_grad, preferred_element_type=jnp.float32))
        part_down = rounded(jnp.dot(weighted_hidden.T, rows_dy, preferred_element_type=jnp.float32))
        return ((totals[0] + part_gate, totals[1] + part_up, totals[2] + part_down), (token_block, route_block))
    start_totals = (jnp.zeros((D, FF), jnp.float32), jnp.zeros((D, FF), jnp.float32), jnp.zeros((FF, D), jnp.float32))
    sums, blocks = lax.scan(one_group, start_totals, (tokens_grouped, grads_grouped, ids_grouped, weights_grouped))
    sum_gate, sum_up, sum_down = sums
    token_grad = blocks[0].reshape(N_GROUP * N_SHARD * TOK_DEV, D)
    route_grad = blocks[1].reshape(N_GROUP * N_SHARD * TOK_DEV, 2)
    square_total = jnp.sum(sum_gate * sum_gate) + jnp.sum(sum_up * sum_up) + jnp.sum(sum_down * sum_down)
    mean_sq = square_total / (3.0 * D * FF)
    inverse_rms = lax.rsqrt(mean_sq + 1e-06)
    return (token_grad, route_grad, (sum_gate * inverse_rms).astype(jnp.bfloat16), (sum_up * inverse_rms).astype(jnp.bfloat16), (sum_down * inverse_rms).astype(jnp.bfloat16), jnp.sqrt(mean_sq))
```

```python
import jax
import jax.numpy as jnp
from jax import lax
from jax.sharding import PartitionSpec as P

CAP = 48
LANES = 128
GATHER_BYTES = 64 << 20


def pack_rows(expert_ids, route_weights):
    expert_hits = expert_ids == 0
    routed = jnp.any(expert_hits, axis=1)
    weight = jnp.sum(
        jnp.where(expert_hits, route_weights.astype(jnp.float32), jnp.float32(0.0)), axis=1
    )
    slot_order = jnp.cumsum(routed.astype(jnp.int32)) - 1
    slot_index = lax.broadcasted_iota(jnp.int32, (CAP, expert_ids.shape[0]), 0)
    placing = jnp.logical_and(slot_order[None, :] == slot_index, routed[None, :])
    return (expert_hits, placing, weight)


def contract_last(left_side, right_side):
    return lax.dot_general(
        left_side, right_side, (((1,), (1,)), ((), ())), preferred_element_type=jnp.float32
    )


def contract_first(left_side, right_side):
    return lax.dot_general(
        left_side, right_side, (((0,), (0,)), ((), ())), preferred_element_type=jnp.float32
    )


def swap(value, axis, offset):
    size = lax.axis_size(axis)
    return lax.ppermute(value, axis, [(i, i ^ offset) for i in range(size)])


def rounded(value):
    return lax.optimization_barrier(value.astype(jnp.bfloat16)).astype(jnp.float32)


def narrow_body(tokens, out_grad, expert_ids, route_weights, w_gate, w_up, w_down):
    expert_hits, placing, weight = pack_rows(expert_ids, route_weights)
    placing_bf = placing.astype(jnp.bfloat16)
    packed_x = jnp.dot(placing_bf, tokens, preferred_element_type=jnp.float32).astype(jnp.bfloat16)
    packed_dy = jnp.dot(placing_bf, out_grad, preferred_element_type=jnp.float32).astype(
        jnp.bfloat16
    )
    packed_route = jnp.sum(placing.astype(jnp.float32) * weight[None, :], axis=1).astype(
        jnp.bfloat16
    )
    rows_x, rows_dy, rows_route = (
        lax.all_gather(packed_x, "shard", axis=0, tiled=True),
        lax.all_gather(packed_dy, "shard", axis=0, tiled=True),
        lax.all_gather(packed_route, "shard", axis=0, tiled=True),
    )
    route_col = rows_route.astype(jnp.float32)[:, None]
    gate_pre = jnp.dot(rows_x, w_gate, preferred_element_type=jnp.float32)
    up_pre = jnp.dot(rows_x, w_up, preferred_element_type=jnp.float32)
    hidden_grad = contract_last(rows_dy, w_down)
    sigmoid_gate = jax.nn.sigmoid(gate_pre)
    activated = gate_pre * sigmoid_gate
    hidden = activated * up_pre
    route_part = jnp.sum(hidden * hidden_grad, axis=1)
    weighted_hidden = (route_col * hidden).astype(jnp.bfloat16)
    gate_grad = (
        route_col * hidden_grad * up_pre * sigmoid_gate * (1.0 + gate_pre * (1.0 - sigmoid_gate))
    ).astype(jnp.bfloat16)
    up_grad = (route_col * hidden_grad * activated).astype(jnp.bfloat16)
    row_grads = contract_last(gate_grad, w_gate) + contract_last(up_grad, w_up)
    back_rows, back_route = (
        lax.psum_scatter(
            row_grads.astype(jnp.bfloat16), "shard", scatter_dimension=0, tiled=True
        ).astype(jnp.float32),
        lax.psum_scatter(
            route_part.astype(jnp.bfloat16), "shard", scatter_dimension=0, tiled=True
        ).astype(jnp.float32),
    )
    token_grad = contract_first(placing_bf, back_rows.astype(jnp.bfloat16)).astype(jnp.bfloat16)
    route_tok = jnp.sum(placing.astype(jnp.float32) * back_route[:, None], axis=0)
    route_grad = jnp.where(expert_hits, route_tok[:, None], jnp.float32(0.0))
    width = w_gate.shape[1]
    own_rows = rows_x.shape[0]
    model_rows = tokens.shape[1] // lax.axis_size("group")
    columns_x, columns_dy = (
        lax.all_to_all(rows_x, "group", split_axis=1, concat_axis=0, tiled=True),
        lax.all_to_all(rows_dy, "group", split_axis=1, concat_axis=0, tiled=True),
    )
    pieces = (
        lax.all_gather(gate_grad, "group", axis=0, tiled=True),
        lax.all_gather(up_grad, "group", axis=0, tiled=True),
        lax.all_gather(weighted_hidden, "group", axis=0, tiled=True),
    )
    row_count = pieces[0].shape[0]
    blocks = row_count // own_rows
    part_x = columns_x.reshape(blocks, own_rows, model_rows)
    part_dy = columns_dy.reshape(blocks, own_rows, model_rows)
    gate_piece = pieces[0].reshape(blocks, own_rows, width)
    up_piece = pieces[1].reshape(blocks, own_rows, width)
    hidden_piece = pieces[2].reshape(blocks, own_rows, width)
    gate_terms = jnp.einsum("krd,krf->kdf", part_x, gate_piece, preferred_element_type=jnp.float32)
    up_terms = jnp.einsum("krd,krf->kdf", part_x, up_piece, preferred_element_type=jnp.float32)
    down_terms = jnp.einsum(
        "krf,krd->kfd", hidden_piece, part_dy, preferred_element_type=jnp.float32
    )
    sum_gate = jnp.sum(rounded(gate_terms), axis=0)
    sum_up = jnp.sum(rounded(up_terms), axis=0)
    sum_down = jnp.sum(rounded(down_terms), axis=0)
    local_sq = (
        jnp.sum(sum_gate * sum_gate) + jnp.sum(sum_up * sum_up) + jnp.sum(sum_down * sum_down)
    )
    square_total = lax.psum(local_sq, ("group", "shard"))
    mean_sq = square_total / (3.0 * tokens.shape[1] * width * lax.axis_size("shard"))
    inverse_rms = lax.rsqrt(mean_sq + 1e-06)
    return (
        token_grad,
        route_grad,
        (sum_gate * inverse_rms).astype(jnp.bfloat16),
        (sum_up * inverse_rms).astype(jnp.bfloat16),
        (sum_down * inverse_rms).astype(jnp.bfloat16),
        jnp.sqrt(mean_sq),
    )


def body(tokens, out_grad, expert_ids, route_weights, w_gate, w_up, w_down):
    groups, shards = lax.axis_size("group"), lax.axis_size("shard")
    columns, rows_ys = groups // 2, shards // 2
    model = tokens.shape[1]
    expert_hits, placing, weight = pack_rows(expert_ids, route_weights)
    placing_bf = placing.astype(jnp.bfloat16)
    packed_x = jnp.dot(placing_bf, tokens, preferred_element_type=jnp.float32).astype(jnp.bfloat16)
    packed_dy = jnp.dot(placing_bf, out_grad, preferred_element_type=jnp.float32).astype(
        jnp.bfloat16
    )
    packed_route = jnp.sum(placing.astype(jnp.float32) * weight[None, :], axis=1).astype(
        jnp.bfloat16
    )
    own = jnp.concatenate(
        [packed_x, packed_dy, jnp.broadcast_to(packed_route[:, None], (CAP, LANES))], axis=1
    )
    piece = {}
    piece[0, 0, 0] = own
    for z in range(1, columns):
        piece[z, 0, 0] = swap(own, "group", 2 * z)
    for z in range(columns):
        for y in range(1, rows_ys):
            piece[z, 0, y] = swap(piece[z, 0, 0], "shard", 2 * y)
        piece[z, 1, 0] = swap(piece[z, 0, 0], "group", 1)
        for y in range(1, rows_ys):
            if (z + y) % 2 == 0:
                piece[z, 1, y] = swap(piece[z, 0, y], "group", 1)
            else:
                piece[z, 1, y] = swap(piece[z, 1, 0], "shard", 2 * y)
    other = {key: swap(value, "shard", 1) for key, value in piece.items()}

    model_rows = model // groups
    own_column = lax.axis_index("group") * model_rows
    sum_gate = sum_up = sum_down = jnp.float32(0.0)
    for z in range(columns):
        parts = []
        for x in range(2):
            for y in range(rows_ys):
                parts += [piece[z, x, y], other[z, x, y]]
        rows = jnp.concatenate(parts, axis=0)
        rows_x, rows_dy = rows[:, :model], rows[:, model : 2 * model]
        route_col = rows[:, 2 * model : 2 * model + 1].astype(jnp.float32)
        gate_pre = jnp.dot(rows_x, w_gate, preferred_element_type=jnp.float32)
        up_pre = jnp.dot(rows_x, w_up, preferred_element_type=jnp.float32)
        hidden_grad = contract_last(rows_dy, w_down)
        sigmoid_gate = jax.nn.sigmoid(gate_pre)
        activated = gate_pre * sigmoid_gate
        hidden = activated * up_pre
        weighted_hidden = (route_col * hidden).astype(jnp.bfloat16)
        routed_grad = route_col * hidden_grad
        gate_grad = (
            routed_grad * up_pre * sigmoid_gate * (1.0 + gate_pre * (1.0 - sigmoid_gate))
        ).astype(jnp.bfloat16)
        up_grad = (routed_grad * activated).astype(jnp.bfloat16)
        if z == 0:
            own_rows = shards * CAP
            route_part = jnp.sum(hidden[:own_rows] * hidden_grad[:own_rows], axis=1)
            row_grads = contract_last(gate_grad[:own_rows], w_gate) + contract_last(
                up_grad[:own_rows], w_up
            )
            returns = jnp.concatenate(
                [
                    row_grads.astype(jnp.bfloat16),
                    jnp.broadcast_to(
                        route_part.astype(jnp.bfloat16)[:, None], (own_rows, LANES)
                    ),
                ],
                axis=1,
            ).reshape(shards, CAP, model + LANES)
            back = returns[0].astype(jnp.float32)
            for s in range(1, shards):
                back = back + swap(returns[s], "shard", s).astype(jnp.float32)
        part_x = lax.dynamic_slice_in_dim(rows, own_column, model_rows, 1)
        part_dy = lax.dynamic_slice_in_dim(rows, model + own_column, model_rows, 1)
        sum_gate = sum_gate + contract_first(part_x, gate_grad)
        sum_up = sum_up + contract_first(part_x, up_grad)
        sum_down = sum_down + contract_first(weighted_hidden, part_dy)

    token_grad = contract_first(placing_bf, back[:, :model].astype(jnp.bfloat16)).astype(
        jnp.bfloat16
    )
    route_tok = jnp.sum(placing.astype(jnp.float32) * back[:, model : model + 1], axis=0)
    route_grad = jnp.where(expert_hits, route_tok[:, None], jnp.float32(0.0))
    local_sq = (
        jnp.sum(sum_gate * sum_gate) + jnp.sum(sum_up * sum_up) + jnp.sum(sum_down * sum_down)
    )
    square_total = lax.psum(local_sq, ("group", "shard"))
    mean_sq = square_total / (3.0 * model * shards * w_gate.shape[1])
    inverse_rms = lax.rsqrt(mean_sq + 1e-06)
    return (
        token_grad,
        route_grad,
        (sum_gate * inverse_rms).astype(jnp.bfloat16),
        (sum_up * inverse_rms).astype(jnp.bfloat16),
        (sum_down * inverse_rms).astype(jnp.bfloat16),
        jnp.sqrt(mean_sq),
    )


def choose(tokens, *rest):
    devices = lax.axis_size("group") * lax.axis_size("shard")
    gathered = devices * CAP * 2 * tokens.shape[1] * tokens.dtype.itemsize
    return (body if gathered <= GATHER_BYTES else narrow_body)(tokens, *rest)


def solution(mesh):
    in_specs = (
        P(("group", "shard"), None),
        P(("group", "shard"), None),
        P(("group", "shard"), None),
        P(("group", "shard"), None),
        P(None, "shard"),
        P(None, "shard"),
        P("shard", None),
    )
    out_specs = (
        P(("group", "shard"), None),
        P(("group", "shard"), None),
        P("group", "shard"),
        P("group", "shard"),
        P("shard", "group"),
        P(),
    )
    return jax.shard_map(choose, mesh=mesh, in_specs=in_specs, out_specs=out_specs, check_vma=False)
```

```python
import jax
import jax.numpy as jnp
from jax import lax
from jax.sharding import PartitionSpec as P

CAP = 48
LANES = 128
GATHER_BYTES = 64 << 20


def pack_rows(expert_ids, route_weights):
    expert_hits = expert_ids == 0
    routed = jnp.any(expert_hits, axis=1)
    weight = jnp.sum(
        jnp.where(expert_hits, route_weights.astype(jnp.float32), jnp.float32(0.0)), axis=1
    )
    slot_order = jnp.cumsum(routed.astype(jnp.int32)) - 1
    slot_index = lax.broadcasted_iota(jnp.int32, (CAP, expert_ids.shape[0]), 0)
    placing = jnp.logical_and(slot_order[None, :] == slot_index, routed[None, :])
    return (expert_hits, placing, weight)


def contract_last(left_side, right_side):
    return lax.dot_general(
        left_side, right_side, (((1,), (1,)), ((), ())), preferred_element_type=jnp.float32
    )


def contract_first(left_side, right_side):
    return lax.dot_general(
        left_side, right_side, (((0,), (0,)), ((), ())), preferred_element_type=jnp.float32
    )


def swap(value, axis, offset):
    size = lax.axis_size(axis)
    return lax.ppermute(value, axis, [(i, i ^ offset) for i in range(size)])


def rounded(value):
    return lax.optimization_barrier(value.astype(jnp.bfloat16)).astype(jnp.float32)


def narrow_body(tokens, out_grad, expert_ids, route_weights, w_gate, w_up, w_down):
    expert_hits, placing, weight = pack_rows(expert_ids, route_weights)
    placing_bf = placing.astype(jnp.bfloat16)
    packed_x = jnp.dot(placing_bf, tokens, preferred_element_type=jnp.float32).astype(jnp.bfloat16)
    packed_dy = jnp.dot(placing_bf, out_grad, preferred_element_type=jnp.float32).astype(
        jnp.bfloat16
    )
    packed_route = jnp.sum(placing.astype(jnp.float32) * weight[None, :], axis=1).astype(
        jnp.bfloat16
    )
    rows_x, rows_dy, rows_route = (
        lax.all_gather(packed_x, "shard", axis=0, tiled=True),
        lax.all_gather(packed_dy, "shard", axis=0, tiled=True),
        lax.all_gather(packed_route, "shard", axis=0, tiled=True),
    )
    route_col = rows_route.astype(jnp.float32)[:, None]
    gate_pre = jnp.dot(rows_x, w_gate, preferred_element_type=jnp.float32)
    up_pre = jnp.dot(rows_x, w_up, preferred_element_type=jnp.float32)
    hidden_grad = contract_last(rows_dy, w_down)
    sigmoid_gate = jax.nn.sigmoid(gate_pre)
    activated = gate_pre * sigmoid_gate
    hidden = activated * up_pre
    route_part = jnp.sum(hidden * hidden_grad, axis=1)
    weighted_hidden = (route_col * hidden).astype(jnp.bfloat16)
    gate_grad = (
        route_col * hidden_grad * up_pre * sigmoid_gate * (1.0 + gate_pre * (1.0 - sigmoid_gate))
    ).astype(jnp.bfloat16)
    up_grad = (route_col * hidden_grad * activated).astype(jnp.bfloat16)
    row_grads = contract_last(gate_grad, w_gate) + contract_last(up_grad, w_up)
    back_rows, back_route = (
        lax.psum_scatter(
            row_grads.astype(jnp.bfloat16), "shard", scatter_dimension=0, tiled=True
        ).astype(jnp.float32),
        lax.psum_scatter(
            route_part.astype(jnp.bfloat16), "shard", scatter_dimension=0, tiled=True
        ).astype(jnp.float32),
    )
    token_grad = contract_first(placing_bf, back_rows.astype(jnp.bfloat16)).astype(jnp.bfloat16)
    route_tok = jnp.sum(placing.astype(jnp.float32) * back_route[:, None], axis=0)
    route_grad = jnp.where(expert_hits, route_tok[:, None], jnp.float32(0.0))
    width = w_gate.shape[1]
    own_rows = rows_x.shape[0]
    model_rows = tokens.shape[1] // lax.axis_size("group")
    columns_x, columns_dy = (
        lax.all_to_all(rows_x, "group", split_axis=1, concat_axis=0, tiled=True),
        lax.all_to_all(rows_dy, "group", split_axis=1, concat_axis=0, tiled=True),
    )
    pieces = (
        lax.all_gather(gate_grad, "group", axis=0, tiled=True),
        lax.all_gather(up_grad, "group", axis=0, tiled=True),
        lax.all_gather(weighted_hidden, "group", axis=0, tiled=True),
    )
    row_count = pieces[0].shape[0]
    blocks = row_count // own_rows
    part_x = columns_x.reshape(blocks, own_rows, model_rows)
    part_dy = columns_dy.reshape(blocks, own_rows, model_rows)
    gate_piece = pieces[0].reshape(blocks, own_rows, width)
    up_piece = pieces[1].reshape(blocks, own_rows, width)
    hidden_piece = pieces[2].reshape(blocks, own_rows, width)
    gate_terms = jnp.einsum("krd,krf->kdf", part_x, gate_piece, preferred_element_type=jnp.float32)
    up_terms = jnp.einsum("krd,krf->kdf", part_x, up_piece, preferred_element_type=jnp.float32)
    down_terms = jnp.einsum(
        "krf,krd->kfd", hidden_piece, part_dy, preferred_element_type=jnp.float32
    )
    sum_gate = jnp.sum(rounded(gate_terms), axis=0)
    sum_up = jnp.sum(rounded(up_terms), axis=0)
    sum_down = jnp.sum(rounded(down_terms), axis=0)
    local_sq = (
        jnp.sum(sum_gate * sum_gate) + jnp.sum(sum_up * sum_up) + jnp.sum(sum_down * sum_down)
    )
    square_total = lax.psum(local_sq, ("group", "shard"))
    mean_sq = square_total / (3.0 * tokens.shape[1] * width * lax.axis_size("shard"))
    inverse_rms = lax.rsqrt(mean_sq + 1e-06)
    return (
        token_grad,
        route_grad,
        (sum_gate * inverse_rms).astype(jnp.bfloat16),
        (sum_up * inverse_rms).astype(jnp.bfloat16),
        (sum_down * inverse_rms).astype(jnp.bfloat16),
        jnp.sqrt(mean_sq),
    )


def body(tokens, out_grad, expert_ids, route_weights, w_gate, w_up, w_down):
    groups, shards = lax.axis_size("group"), lax.axis_size("shard")
    columns, rows_ys = groups // 2, shards // 2
    model = tokens.shape[1]
    expert_hits, placing, weight = pack_rows(expert_ids, route_weights)
    placing_bf = placing.astype(jnp.bfloat16)
    packed_x = jnp.dot(placing_bf, tokens, preferred_element_type=jnp.float32).astype(jnp.bfloat16)
    packed_dy = jnp.dot(placing_bf, out_grad, preferred_element_type=jnp.float32).astype(
        jnp.bfloat16
    )
    packed_route = jnp.sum(placing.astype(jnp.float32) * weight[None, :], axis=1).astype(
        jnp.bfloat16
    )
    own = jnp.concatenate(
        [packed_x, packed_dy, jnp.broadcast_to(packed_route[:, None], (CAP, LANES))], axis=1
    )
    piece = {}
    piece[0, 0, 0] = own
    for z in range(1, columns):
        piece[z, 0, 0] = swap(own, "group", 2 * z)
    for z in range(columns):
        for y in range(1, rows_ys):
            piece[z, 0, y] = swap(piece[z, 0, 0], "shard", 2 * y)
        piece[z, 1, 0] = swap(piece[z, 0, 0], "group", 1)
        for y in range(1, rows_ys):
            if (z + y) % 2 == 0:
                piece[z, 1, y] = swap(piece[z, 0, y], "group", 1)
            else:
                piece[z, 1, y] = swap(piece[z, 1, 0], "shard", 2 * y)
    other = {key: swap(value, "shard", 1) for key, value in piece.items()}

    model_rows = model // groups
    own_column = lax.axis_index("group") * model_rows
    sum_gate = sum_up = sum_down = jnp.float32(0.0)
    for chunk in ((0,), tuple(range(1, columns))):
        parts = []
        for z in chunk:
            for x in range(2):
                for y in range(rows_ys):
                    parts += [piece[z, x, y], other[z, x, y]]
        rows = jnp.concatenate(parts, axis=0)
        rows_x, rows_dy = rows[:, :model], rows[:, model : 2 * model]
        route_col = rows[:, 2 * model : 2 * model + 1].astype(jnp.float32)
        gate_pre = jnp.dot(rows_x, w_gate, preferred_element_type=jnp.float32)
        up_pre = jnp.dot(rows_x, w_up, preferred_element_type=jnp.float32)
        hidden_grad = contract_last(rows_dy, w_down)
        sigmoid_gate = jax.nn.sigmoid(gate_pre)
        activated = gate_pre * sigmoid_gate
        hidden = activated * up_pre
        weighted_hidden = (route_col * hidden).astype(jnp.bfloat16)
        routed_grad = route_col * hidden_grad
        gate_grad = (
            routed_grad * up_pre * sigmoid_gate * (1.0 + gate_pre * (1.0 - sigmoid_gate))
        ).astype(jnp.bfloat16)
        up_grad = (routed_grad * activated).astype(jnp.bfloat16)
        if chunk[0] == 0:
            own_rows = shards * CAP
            route_part = jnp.sum(hidden[:own_rows] * hidden_grad[:own_rows], axis=1)
            row_grads = contract_last(gate_grad[:own_rows], w_gate) + contract_last(
                up_grad[:own_rows], w_up
            )
            returns = jnp.concatenate(
                [
                    row_grads.astype(jnp.bfloat16),
                    jnp.broadcast_to(
                        route_part.astype(jnp.bfloat16)[:, None], (own_rows, LANES)
                    ),
                ],
                axis=1,
            ).reshape(shards, CAP, model + LANES)
            back = returns[0].astype(jnp.float32)
            for s in range(1, shards):
                back = back + swap(returns[s], "shard", s).astype(jnp.float32)
        part_x = lax.dynamic_slice_in_dim(rows, own_column, model_rows, 1)
        part_dy = lax.dynamic_slice_in_dim(rows, model + own_column, model_rows, 1)
        sum_gate = sum_gate + contract_first(part_x, gate_grad)
        sum_up = sum_up + contract_first(part_x, up_grad)
        sum_down = sum_down + contract_first(weighted_hidden, part_dy)

    token_grad = contract_first(placing_bf, back[:, :model].astype(jnp.bfloat16)).astype(
        jnp.bfloat16
    )
    route_tok = jnp.sum(placing.astype(jnp.float32) * back[:, model : model + 1], axis=0)
    route_grad = jnp.where(expert_hits, route_tok[:, None], jnp.float32(0.0))
    local_sq = (
        jnp.sum(sum_gate * sum_gate) + jnp.sum(sum_up * sum_up) + jnp.sum(sum_down * sum_down)
    )
    square_total = lax.psum(local_sq, ("group", "shard"))
    mean_sq = square_total / (3.0 * model * shards * w_gate.shape[1])
    inverse_rms = lax.rsqrt(mean_sq + 1e-06)
    return (
        token_grad,
        route_grad,
        (sum_gate * inverse_rms).astype(jnp.bfloat16),
        (sum_up * inverse_rms).astype(jnp.bfloat16),
        (sum_down * inverse_rms).astype(jnp.bfloat16),
        jnp.sqrt(mean_sq),
    )


def choose(tokens, *rest):
    devices = lax.axis_size("group") * lax.axis_size("shard")
    gathered = devices * CAP * 2 * tokens.shape[1] * tokens.dtype.itemsize
    return (body if gathered <= GATHER_BYTES else narrow_body)(tokens, *rest)


def solution(mesh):
    in_specs = (
        P(("group", "shard"), None),
        P(("group", "shard"), None),
        P(("group", "shard"), None),
        P(("group", "shard"), None),
        P(None, "shard"),
        P(None, "shard"),
        P("shard", None),
    )
    out_specs = (
        P(("group", "shard"), None),
        P(("group", "shard"), None),
        P("group", "shard"),
        P("group", "shard"),
        P("shard", "group"),
        P(),
    )
    return jax.shard_map(choose, mesh=mesh, in_specs=in_specs, out_specs=out_specs, check_vma=False)
```
